128 devices in a mesh: dp: 1, sp: 128 (over z, y, x, core).
Axes of the slice: x: 4, y: 4, z: 4, core: 2. Of those that a mesh axis runs over, the one named last changes fastest.
Arguments:
- x_patch: bfloat16 [32, 16384, 512], P('dp', 'sp')
- w_tok1: bfloat16 [16384, 256], P('sp')
- b_tok1: float32 [256], P('sp')
- w_tok2: bfloat16 [256, 16384], P(None, 'sp')
- b_tok2: float32 [16384], P('sp')
- w_ch1: bfloat16 [512, 2048], replicated
- b_ch1: float32 [2048], replicated
- w_ch2: bfloat16 [2048, 512], replicated
- b_ch2: float32 [512], replicated
- ln1_gain: float32 [512], replicated
- ln1_bias: float32 [512], replicated
- ln2_gain: float32 [512], replicated
- ln2_bias: float32 [512], replicated
Outputs:
- output: bfloat16 [32, 16384, 512], P('dp', 'sp')
All inputs are finite; a program needn't handle non-finite values.
Results may differ from the reference program's by a relative error of at most 0.00982353.
Values are sent between devices in bfloat16 or wider.
A program may use at most 1 GiB of HBM per device.

```python
import jax
import jax.numpy as jnp
from jax import lax

BATCH = 32
PATCHES = 16384
CHANNELS = 512
TOKEN_HID = 256
CHAN_HID = 2048
LN_EPS = 1e-6


def draw_normal(rng_key, out_shape, spread):
    return jax.random.normal(rng_key, out_shape, jnp.float32) * spread


def setup_inputs(seed: int = 0, part: int = 0) -> dict:
    shared = jax.random.split(jax.random.key(seed), 12)
    x_key = jax.random.fold_in(jax.random.key(seed + 1), part)
    x_patch = jax.random.normal(x_key, (BATCH, PATCHES, CHANNELS), jnp.float32)
    return {
        "x_patch": x_patch.astype(jnp.bfloat16),
        "w_tok1": draw_normal(shared[0], (PATCHES, TOKEN_HID), PATCHES ** -0.5).astype(jnp.bfloat16),
        "b_tok1": draw_normal(shared[1], (TOKEN_HID,), 0.5),
        "w_tok2": draw_normal(shared[2], (TOKEN_HID, PATCHES), TOKEN_HID ** -0.5).astype(jnp.bfloat16),
        "b_tok2": draw_normal(shared[3], (PATCHES,), 0.5),
        "w_ch1": draw_normal(shared[4], (CHANNELS, CHAN_HID), CHANNELS ** -0.5).astype(jnp.bfloat16),
        "b_ch1": draw_normal(shared[5], (CHAN_HID,), 0.5),
        "w_ch2": draw_normal(shared[6], (CHAN_HID, CHANNELS), CHAN_HID ** -0.5).astype(jnp.bfloat16),
        "b_ch2": draw_normal(shared[7], (CHANNELS,), 0.3),
        "ln1_gain": 1.0 + draw_normal(shared[8], (CHANNELS,), 0.2),
        "ln1_bias": draw_normal(shared[9], (CHANNELS,), 0.3),
        "ln2_gain": 1.0 + draw_normal(shared[10], (CHANNELS,), 0.2),
        "ln2_bias": draw_normal(shared[11], (CHANNELS,), 0.3),
    }


def layer_norm(values, ln_gain, ln_bias):
    mean_val = jnp.mean(values, axis=-1, keepdims=True)
    centred = values - mean_val
    var_val = jnp.mean(centred * centred, axis=-1, keepdims=True)
    return centred * lax.rsqrt(var_val + LN_EPS) * ln_gain + ln_bias


def reference(x_patch, w_tok1, b_tok1, w_tok2, b_tok2, w_ch1, b_ch1, w_ch2, b_ch2, ln1_gain, ln1_bias, ln2_gain, ln2_bias):
    def one_image(x_img):
        x_wide = x_img.astype(jnp.float32)
        normed = layer_norm(x_wide, ln1_gain, ln1_bias).astype(jnp.bfloat16)
        tok_pre = jnp.dot(w_tok1.T, normed, preferred_element_type=jnp.float32) + b_tok1[:, None]
        tok_act = jax.nn.gelu(tok_pre).astype(jnp.bfloat16)
        tok_out = jnp.dot(w_tok2.T, tok_act, preferred_element_type=jnp.float32) + b_tok2[:, None]
        x_mid = (x_wide + tok_out).astype(jnp.bfloat16)
        mid_wide = x_mid.astype(jnp.float32)
        normed_two = layer_norm(mid_wide, ln2_gain, ln2_bias).astype(jnp.bfloat16)
        ch_pre = jnp.dot(normed_two, w_ch1, preferred_element_type=jnp.float32) + b_ch1
        ch_act = jax.nn.gelu(ch_pre).astype(jnp.bfloat16)
        ch_out = jnp.dot(ch_act, w_ch2, preferred_element_type=jnp.float32) + b_ch2
        return (mid_wide + ch_out).astype(jnp.bfloat16)

    return lax.map(one_image, x_patch)
```

```python
import functools

import jax
import jax.numpy as jnp
from jax import lax
from jax.experimental import pallas as pl
from jax.experimental.pallas import tpu as pltpu
from jax.sharding import PartitionSpec as P

LN_EPS = 1e-6
F32 = jnp.float32
BF16 = jnp.bfloat16
HALF = (pl.ds(0, 256), pl.ds(256, 256))
CHUNKS = (
    ("xyz", "yzx"),
    ("yzx", "zxy"),
    ("zxy", "xyz"),
    ("xyz", "xzy"),
)
K = len(CHUNKS)


def layer_norm(values, ln_gain, ln_bias):
    mean_val = jnp.mean(values, axis=-1, keepdims=True)
    centred = values - mean_val
    var_val = jnp.mean(centred * centred, axis=-1, keepdims=True)
    return centred * lax.rsqrt(var_val + LN_EPS) * ln_gain + ln_bias


def gelu(a):
    return 0.5 * a * (1.0 + jnp.tanh(0.7978845608028654 * (a + 0.044715 * (a * a * a))))


def token_kernel(
    x_hbm, w1_ref, b1_ref, gain_ref, bias_ref, g_hbm,
    xv, w1o, w1t, tile_in, tile_all, usend, ustage, uall, relay, hb, rq0, rd0, rs0, hq, rq1, rd1, rs1, gall,
    send_sems, recv_sems, local_sems,
):
    me = lax.axis_index("sp")
    co = {"z": me // 32, "y": (me // 8) % 4, "x": (me // 2) % 4}
    core = me % 2
    other = 1 - core

    def device(c=None, **at):
        z, y, x = (at.get(a, co[a]) for a in "zyx")
        return ((z * 4 + y) * 4 + x) * 2 + (core if c is None else c)

    def near(axis, step):
        return device(**{axis: (co[axis] + step) % 4})

    sent = []

    def send(src, dst, to):
        n = len(sent)
        copy = pltpu.make_async_remote_copy(
            src_ref=src, dst_ref=dst, send_sem=send_sems.at[n], recv_sem=recv_sems.at[n],
            device_id={"sp": to}, device_id_type=pl.DeviceIdType.MESH,
        )
        copy.start()
        sent.append(copy)
        return copy

    loads = []
    for k in range(K):
        load = pltpu.make_async_copy(x_hbm.at[pl.ds(8 * k, 8)], xv.at[pl.ds(8 * k, 8)], local_sems.at[k])
        load.start()
        loads.append(load)

    partner = device(c=other)
    group = [device(c=(core + j) % 2, x=(co["x"] + s) % 4) for s in range(4) for j in range(2) if (s, j) != (0, 0)]
    peers = group + [near(a, s) for a in "yz" for s in (1, 2, 3)]
    barrier = pltpu.get_barrier_semaphore()
    for peer in peers:
        pl.semaphore_signal(barrier, inc=1, device_id={"sp": peer}, device_id_type=pl.DeviceIdType.MESH)
    pl.semaphore_wait(barrier, len(peers))

    w1o[...] = w1_ref[...].T
    w1_in = {}
    def lanes(pos, c):
        return pl.ds(pl.multiple_of((pos * 2 + c) * 128, 128), 128)
    for i, a in enumerate("xyz"):
        w1t[i, :, lanes(co[a], core)] = w1o[...]
        dst = w1t.at[i, :, lanes(co[a], core)]
        w1_in[a] = [send(w1o, dst, near(a, s)) for s in (1, 2, 3)] + [send(w1o, dst, partner)]

    row = lax.broadcasted_iota(jnp.int32, (16, 128), 0)
    slot = co["x"] * 2 + core
    tile_in[8] = jnp.where(row == 2 * slot, b1_ref[0], jnp.where(row == 2 * slot + 1, b1_ref[1], 0.0))
    tile_in[slot] = tile_in[8]
    b1_in = [send(tile_in.at[8], tile_in.at[slot], to) for to in group]

    gain, bias = gain_ref[...], bias_ref[...]
    pairs = []

    def norm(k):
        loads[k].wait()

        def body(i, carry):
            mine = layer_norm(xv[8 * k + 4 * core + i].astype(F32), gain, bias).astype(BF16)
            ustage[k, i, core] = mine
            theirs = layer_norm(xv[8 * k + 4 * other + i].astype(F32), gain, bias).astype(BF16)
            usend[k, i] = theirs
            return carry

        lax.fori_loop(0, 4, body, 0)
        return send(usend.at[k], ustage.at[k, :, core], partner)

    def exchange(k, pair):
        pair.wait_recv()
        a = CHUNKS[k][0][0]
        p = co[a]
        right, left = near(a, 1), near(a, 3)
        opp, rt, lf = (p + 2) % 4, (p + 1) % 4, (p + 3) % 4
        passing = [
            send(ustage.at[k, opp, :, :, HALF[0]], relay.at[k, 0], right),
            send(ustage.at[k, opp, :, :, HALF[1]], relay.at[k, 1], left),
        ]
        direct = [
            send(ustage.at[k, rt], uall.at[k, p], right),
            send(ustage.at[k, lf], uall.at[k, p], left),
        ]
        uall[k, p] = ustage[k, p]
        return passing, direct

    def pass_on(k, state):
        passing, direct = state
        a = CHUNKS[k][0][0]
        p = co[a]
        passing[0].wait_recv()
        direct.append(send(relay.at[k, 0], uall.at[k, (p + 3) % 4, :, :, HALF[0]], near(a, 1)))
        passing[1].wait_recv()
        direct.append(send(relay.at[k, 1], uall.at[k, (p + 1) % 4, :, :, HALF[1]], near(a, 3)))
        return direct

    def ring_first(a, part, in_opp, in_near):
        q = co[a]
        right, left = near(a, 1), near(a, 3)
        opp, rt, lf = (q + 2) % 4, (q + 1) % 4, (q + 3) % 4
        first = [send(part(opp, HALF[0]), in_opp.at[0], right), send(part(opp, HALF[1]), in_opp.at[1], left)]
        straight = [send(part(rt, HALF[1]), in_near.at[0], right), send(part(lf, HALF[0]), in_near.at[1], left)]
        return first, straight

    def ring_second(a, part, in_opp, in_sum, first):
        q = co[a]
        right, left = near(a, 1), near(a, 3)
        rt, lf = (q + 1) % 4, (q + 3) % 4
        out = []
        for j, (pos, to) in enumerate(((rt, right), (lf, left))):
            first[j].wait_recv()
            ref = part(pos, HALF[j])
            ref[...] = ref[...] + in_opp[j]
            out.append(send(ref, in_sum.at[j], to))
        return out

    def ring_last(a, part, in_near, in_sum, straight, second):
        q = co[a]
        for copy in straight + second:
            copy.wait_recv()
        low = part(q, HALF[0])[...] + in_near[1] + in_sum[0]
        high = part(q, HALF[1])[...] + in_near[0] + in_sum[1]
        return low, high

    def part_q(k):
        return lambda pos, half: hb.at[k, :, pos, :, half]

    def part_r(k):
        return lambda pos, half: hq.at[k, pos, :, half]

    def mix(k, direct):
        for copy in direct:
            copy.wait_recv()
        axes = CHUNKS[k][0]
        u = uall[k].reshape(1024, 512)
        part = jnp.dot(w1t["xyz".index(axes[0])], u, preferred_element_type=F32)
        hb[k] = part.reshape(4, 4, 16, 512)
        return ring_first(axes[1], part_q(k), rq0.at[k], rd0.at[k])

    def sum_q(k, state):
        first, straight = state
        return straight, ring_second(CHUNKS[k][0][1], part_q(k), rq0.at[k], rs0.at[k], first)

    def start_r(k, state):
        axes = CHUNKS[k][0]
        low, high = ring_last(axes[1], part_q(k), rd0.at[k], rs0.at[k], *state)
        hq[k, :, :, HALF[0]] = low
        hq[k, :, :, HALF[1]] = high
        return ring_first(axes[2], part_r(k), rq1.at[k], rd1.at[k])

    def sum_r(k, state):
        first, straight = state
        return straight, ring_second(CHUNKS[k][0][2], part_r(k), rq1.at[k], rs1.at[k], first)

    def block(k, known):
        at = [slice(None) if a in known else co[a] for a in (CHUNKS[k][0][0], CHUNKS[k][0][2], CHUNKS[k][0][1])]
        return lambda axis=None, pos=None, half=slice(None): gall.at[
            (k, core) + tuple(pos if a == axis else v for a, v in zip(CHUNKS[k][0][0] + CHUNKS[k][0][2] + CHUNKS[k][0][1], at))
            + (slice(None), half)
        ]

    def activate(k, state):
        axes = CHUNKS[k][0]
        low, high = ring_last(axes[2], part_r(k), rd1.at[k], rs1.at[k], *state)
        tile = tile_all[co[axes[2]], co[axes[1]]]
        shift = jnp.concatenate([tile, tile], axis=1)
        where = (k, core, co[axes[0]], co[axes[2]], co[axes[1]])
        gall[where + (slice(None), HALF[0])] = gelu(low + shift).astype(BF16)
        gall[where + (slice(None), HALF[1])] = gelu(high + shift).astype(BF16)
        a = CHUNKS[k][1][0]
        own = block(k, "")()
        return [send(own, own, near(a, s)) for s in (1, 3, 2)]

    def gather(k, n, waits):
        for copy in waits:
            copy.wait_recv()
        a = CHUNKS[k][1][n]
        own = block(k, CHUNKS[k][1][:n])()
        return [send(own, own, near(a, 1)), send(own, own, near(a, 3))]

    def gather_on(k, n, waits):
        a = CHUNKS[k][1][n]
        at = block(k, CHUNKS[k][1][:n])
        out = list(waits)
        for j, (pos, to) in enumerate((((co[a] + 3) % 4, near(a, 1)), ((co[a] + 1) % 4, near(a, 3)))):
            waits[j].wait_recv()
            ref = at(a, pos, HALF[j])
            out.append(send(ref, ref, to))
        return out[2:]

    def share(k, waits):
        for copy in waits:
            copy.wait_recv()
        return send(gall.at[k, core], gall.at[k, core], partner)

    def write(k, copy):
        copy.wait_recv()
        out = pltpu.make_async_copy(gall.at[k], g_hbm.at[k], local_sems.at[K + k])
        out.start()
        return out

    state = [norm(k) for k in range(K)]
    state = [exchange(k, s) for k, s in enumerate(state)]

    for copy in b1_in:
        copy.wait_recv()
    tile = tile_in[0]
    for j in range(1, 8):
        tile = tile + tile_in[j]
    tile_all[co["z"], co["y"]] = tile
    ref = tile_all.at[co["z"], co["y"]]
    b1_in = [send(ref, ref, near("y", s)) for s in (1, 2, 3)]
    w1_share = []
    for i, a in enumerate("xyz"):
        for s, copy in zip((3, 2, 1), w1_in[a]):
            copy.wait_recv()
            ref = w1t.at[i, :, lanes((co[a] + s) % 4, core)]
            w1_share.append(send(ref, ref, partner))
        w1_share.append(w1_in[a][3])
    for copy in b1_in:
        copy.wait_recv()
    ref = tile_all.at[co["z"]]
    b1_in = [send(ref, ref, near("z", s)) for s in (1, 2, 3)]
    for copy in w1_share + b1_in:
        copy.wait_recv()

    for step in (pass_on, mix, sum_q, start_r, sum_r, activate):
        state = [step(k, s) for k, s in enumerate(state)]
    for n in (1, 2):
        state = [gather(k, n, s) for k, s in enumerate(state)]
        state = [gather_on(k, n, s) for k, s in enumerate(state)]
    state = [share(k, s) for k, s in enumerate(state)]
    state = [write(k, s) for k, s in enumerate(state)]
    for copy in state:
        copy.wait()
    for copy in sent:
        copy.wait_send()


N_COPIES = 31 * K + 12 + 7 + 3 + 9 + 3


def token_hidden(x, w1, b1, gain, bias):
    any_space = pl.BlockSpec(memory_space=pl.ANY)
    vmem = pl.BlockSpec(memory_space=pltpu.VMEM)
    out = pl.pallas_call(
        token_kernel,
        name="token_hidden",
        out_shape=jax.ShapeDtypeStruct((K, 2, 4, 4, 4, 16, 512), BF16),
        in_specs=[any_space, vmem, pl.BlockSpec(memory_space=pltpu.SMEM), vmem, vmem],
        out_specs=any_space,
        scratch_shapes=[
            pltpu.VMEM((32, 128, 512), BF16),
            pltpu.VMEM((256, 128), BF16),
            pltpu.VMEM((3, 256, 1024), BF16),
            pltpu.VMEM((9, 16, 128), F32),
            pltpu.VMEM((4, 4, 16, 128), F32),
            pltpu.VMEM((K, 4, 128, 512), BF16),
            pltpu.VMEM((K, 4, 2, 128, 512), BF16),
            pltpu.VMEM((K, 4, 2, 128, 512), BF16),
            pltpu.VMEM((K, 2, 2, 128, 256), BF16),
            pltpu.VMEM((K, 4, 4, 16, 512), F32),
            pltpu.VMEM((K, 2, 4, 16, 256), F32),
            pltpu.VMEM((K, 2, 4, 16, 256), F32),
            pltpu.VMEM((K, 2, 4, 16, 256), F32),
            pltpu.VMEM((K, 4, 16, 512), F32),
            pltpu.VMEM((K, 2, 16, 256), F32),
            pltpu.VMEM((K, 2, 16, 256), F32),
            pltpu.VMEM((K, 2, 16, 256), F32),
            pltpu.VMEM((K, 2, 4, 4, 4, 16, 512), BF16),
            pltpu.SemaphoreType.DMA((N_COPIES,)),
            pltpu.SemaphoreType.DMA((N_COPIES,)),
            pltpu.SemaphoreType.DMA((2 * K,)),
        ],
        compiler_params=pltpu.CompilerParams(
            collective_id=0, has_side_effects=True, vmem_limit_bytes=60 * 1024 * 1024
        ),
    )(x, w1, b1, gain.reshape(1, 512), bias.reshape(1, 512))
    return out.reshape(32, 256, 512)


def channel_mix(x_mid, w_ch1, b_ch1, w_ch2, b_ch2, ln2_gain, ln2_bias):
    mid_wide = x_mid.astype(jnp.float32)
    normed_two = layer_norm(mid_wide, ln2_gain, ln2_bias).astype(jnp.bfloat16)
    ch_pre = jnp.einsum("bsc,cf->bsf", normed_two, w_ch1, preferred_element_type=jnp.float32) + b_ch1
    ch_act = jax.nn.gelu(ch_pre).astype(jnp.bfloat16)
    ch_out = jnp.einsum("bsf,fc->bsc", ch_act, w_ch2, preferred_element_type=jnp.float32) + b_ch2
    return (mid_wide + ch_out).astype(jnp.bfloat16)


def solution(mesh):
    row_spec = P("dp", "sp", None)

    def local_layer(x_blk, w1_rows, b1_part, w2_cols, b2_part, w_ch1, b_ch1, w_ch2, b_ch2, ln1_gain, ln1_bias, ln2_gain, ln2_bias):
        act_full = token_hidden(x_blk, w1_rows, b1_part, ln1_gain, ln1_bias)
        tok_out = jnp.einsum("bdc,ds->bsc", act_full, w2_cols, preferred_element_type=jnp.float32) + b2_part[None, :, None]
        x_mid = (x_blk.astype(jnp.float32) + tok_out).astype(jnp.bfloat16)
        return channel_mix(x_mid, w_ch1, b_ch1, w_ch2, b_ch2, ln2_gain, ln2_bias)

    in_specs = (row_spec, P("sp", None), P("sp"), P(None, "sp"), P("sp"), P(None, None), P(None), P(None, None), P(None), P(None), P(None), P(None), P(None))
    return jax.shard_map(local_layer, mesh=mesh, in_specs=in_specs, out_specs=row_spec, check_vma=False)
```

```python
import jax
import jax.numpy as jnp
from jax import lax
from jax.experimental import pallas as pl
from jax.experimental.pallas import tpu as pltpu
from jax.sharding import PartitionSpec as P

LN_EPS = 1e-6
F32 = jnp.float32
BF16 = jnp.bfloat16
MESH = pl.DeviceIdType.MESH
PIECES = (
    ("xyz", "xyz"),
    ("yzx", "yxz"),
    ("zxy", "zyx"),
    ("xyz", "xzy"),
    ("yzx", "yxz"),
    ("zxy", "zyx"),
    ("xyz", "xyz"),
    ("yxz", "yxz"),
)
N = len(PIECES)
K = N // 2
STEP = 3
ROWS = 2
BLOCKS = 32 // ROWS
C0 = 0.7978845608028654
C1 = C0 * 0.044715


def layer_norm(values, ln_gain, ln_bias):
    mean_val = jnp.mean(values, axis=-1, keepdims=True)
    centred = values - mean_val
    var_val = jnp.mean(centred * centred, axis=-1, keepdims=True)
    return centred * lax.rsqrt(var_val + LN_EPS) * ln_gain + ln_bias


def gelu(a):
    half = 0.5 * a
    return half + half * jnp.tanh(a * (C0 + C1 * (a * a)))


def mixer_kernel(
    x_hbm, w1_ref, b1_ref, w2_ref, b2_ref, wc1_hbm, bc1_ref, wc2_hbm, bc2_ref, g1_ref, h1_ref, g2_ref, h2_ref, z_hbm,
    xv, w1o, w1t, w2t, b2c, wc1, wc2, tile_in, tile_all, usend, ustage, uall, relay, hb, rq, rd, rs, hq, rr, gall,
    send_sems, recv_sems, local_sems,
):
    me = lax.axis_index("sp")
    co = {"z": me // 32, "y": (me // 8) % 4, "x": (me // 2) % 4}
    core = me % 2
    other = 1 - core

    def device(c=None, **at):
        z, y, x = (at.get(a, co[a]) for a in "zyx")
        return ((z * 4 + y) * 4 + x) * 2 + (core if c is None else c)

    hop = {a: [co[a]] + [(co[a] + s) % 4 for s in (1, 2, 3)] for a in "xyz"}
    near = {a: [None] + [device(**{a: hop[a][s]}) for s in (1, 2, 3)] for a in "xyz"}
    partner = device(c=other)
    group = [device(c=(core + j) % 2, x=hop["x"][s]) for s in range(4) for j in range(2) if (s, j) != (0, 0)]
    sent = []

    def remote(src, dst, to):
        n = len(sent)
        copy = pltpu.make_async_remote_copy(
            src_ref=src, dst_ref=dst, send_sem=send_sems.at[n], recv_sem=recv_sems.at[n],
            device_id={"sp": to}, device_id_type=MESH,
        )
        sent.append(copy)
        return copy

    def start(copies):
        for copy in copies:
            copy.start()

    def arrive(copies):
        for copy in copies:
            copy.wait_recv()

    def local(src, dst, n):
        return pltpu.make_async_copy(src, dst, local_sems.at[n])

    loads = [local(x_hbm.at[pl.ds(8 * k, 8)], xv.at[pl.ds(8 * k, 8)], k) for k in range(K)]
    loads += [local(wc1_hbm, wc1, K), local(wc2_hbm, wc2, K + 1)]

    def lanes(pos, c):
        return pl.ds(pl.multiple_of((pos * 2 + c) * 128, 128), 128)

    w1_ring, w1_mine, w1_share = {}, {}, {}
    for i, a in enumerate("xyz"):
        dst = w1t.at[i, :, lanes(co[a], core)]
        w1_ring[a] = [remote(w1o, dst, near[a][s]) for s in (1, 2, 3)]
        w1_mine[a] = remote(w1o, dst, partner)
        refs = [w1t.at[i, :, lanes(hop[a][s], core)] for s in (3, 2, 1)]
        w1_share[a] = [remote(ref, ref, partner) for ref in refs]
    slot = co["x"] * 2 + core
    b1_group = [remote(tile_in.at[8], tile_in.at[slot], to) for to in group]
    ref = tile_all.at[co["z"], co["y"]]
    b1_y = [remote(ref, ref, near["y"][s]) for s in (1, 2, 3)]
    ref = tile_all.at[co["z"]]
    b1_z = [remote(ref, ref, near["z"][s]) for s in (1, 2, 3)]
    pairs = [remote(usend.at[k], ustage.at[k, :, core], partner) for k in range(K)]

    class Piece:
        pass

    pieces = []
    for j, (axes, order) in enumerate(PIECES):
        s = Piece()
        s.k, s.h, s.axes, s.order = j // 2, j % 2, axes, order
        a, b, c = axes
        low = s.h * 256
        s.half = half = (pl.ds(low, 128), pl.ds(low + 128, 128))
        s.lanes = pl.ds(low, 256)
        s.at = (co[a], co[c], co[b])
        p, st = hop[a], ustage.at[s.k]
        s.passing = [
            remote(st.at[p[2], :, :, half[0]], relay.at[j, 0], near[a][1]),
            remote(st.at[p[2], :, :, half[1]], relay.at[j, 1], near[a][3]),
        ]
        s.direct = [
            remote(st.at[p[1], :, :, s.lanes], uall.at[j, p[0]], near[a][1]),
            remote(st.at[p[3], :, :, s.lanes], uall.at[j, p[0]], near[a][3]),
        ]
        s.forward = [
            remote(relay.at[j, 0], uall.at[j, p[3], :, :, pl.ds(0, 128)], near[a][1]),
            remote(relay.at[j, 1], uall.at[j, p[1], :, :, pl.ds(128, 128)], near[a][3]),
        ]
        q = hop[b]
        s.part = lambda pos, i, j=j: hb.at[j, :, pos, :, pl.ds(128 * i, 128)]
        s.first = [remote(s.part(q[2], 0), rq.at[j, 0], near[b][1]), remote(s.part(q[2], 1), rq.at[j, 1], near[b][3])]
        s.straight = [remote(s.part(q[1], 1), rd.at[j, 0], near[b][1]), remote(s.part(q[3], 0), rd.at[j, 1], near[b][3])]
        s.second = [remote(s.part(q[1], 0), rs.at[j, 0], near[b][1]), remote(s.part(q[3], 1), rs.at[j, 1], near[b][3])]
        s.last = [remote(hq.at[j, hop[c][d]], rr.at[j, d], near[c][d]) for d in (1, 3, 2)]

        def block(known, axis=None, pos=None, lane=None, s=s):
            names = (s.axes[0], s.axes[2], s.axes[1])
            at = tuple(pos if n == axis else slice(None) if n in known else v for n, v in zip(names, s.at))
            return gall.at[(s.k, core) + at + (slice(None), s.lanes if lane is None else s.half[lane])]

        d0, d1, d2 = order
        own = block("")
        s.gather0 = [remote(own, own, near[d0][d]) for d in (1, 3, 2)]
        own = block(d0)
        s.gather1 = [remote(own, own, near[d1][d]) for d in (1, 3, 2)]
        own = block(d0 + d1)
        s.gather2 = [remote(own, own, near[d2][1]), remote(own, own, near[d2][3])]
        ends = [block(d0 + d1, d2, hop[d2][3], 0), block(d0 + d1, d2, hop[d2][1], 1)]
        s.gather3 = [remote(ends[0], ends[0], near[d2][1]), remote(ends[1], ends[1], near[d2][3])]
        whole = gall.at[s.k, core, :, :, :, :, s.lanes]
        s.share = remote(whole, whole, partner)
        pieces.append(s)

    gain1, bias1 = g1_ref[...], h1_ref[...]

    def norm(k):
        loads[k].wait()

        def body(i, carry):
            mine = layer_norm(xv[8 * k + 4 * core + i].astype(F32), gain1, bias1).astype(BF16)
            ustage[k, i, core] = mine
            theirs = layer_norm(xv[8 * k + 4 * other + i].astype(F32), gain1, bias1).astype(BF16)
            usend[k, i] = theirs
            return carry

        lax.fori_loop(0, 4, body, 0)
        pairs[k].start()

    def exchange(j, s):
        if s.h == 0:
            pairs[s.k].wait_recv()
        start(s.passing)
        start(s.direct)
        uall[j, s.at[0]] = ustage[s.k, s.at[0], :, :, s.lanes]

    def pass_on(j, s):
        for came, go in zip(s.passing, s.forward):
            came.wait_recv()
            go.start()

    def mix(j, s):
        arrive(s.direct + s.forward)
        u = uall[j].reshape(1024, 256)
        part = jnp.dot(w1t["xyz".index(s.axes[0])], u, preferred_element_type=F32)
        hb[j] = part.reshape(4, 4, 16, 256)
        start(s.first + s.straight)

    def sum_q(j, s):
        q = hop[s.axes[1]]
        for i, pos in enumerate((q[1], q[3])):
            s.first[i].wait_recv()
            ref = s.part(pos, i)
            ref[...] = ref[...] + rq[j, i]
            s.second[i].start()

    def start_r(j, s):
        arrive(s.straight + s.second)
        q = co[s.axes[1]]
        hq[j, :, :, pl.ds(0, 128)] = s.part(q, 0)[...] + rd[j, 1] + rs[j, 0]
        hq[j, :, :, pl.ds(128, 128)] = s.part(q, 1)[...] + rd[j, 0] + rs[j, 1]
        start(s.last)

    def activate(j, s):
        arrive(s.last)
        a, b, c = s.axes
        tile = tile_all[co[c], co[b]]
        total = hq[j, co[c]] + rr[j, 1] + rr[j, 2] + rr[j, 3] + jnp.concatenate([tile, tile], axis=1)
        gall[s.k, core, s.at[0], s.at[1], s.at[2], :, s.lanes] = gelu(total).astype(BF16)
        start(s.gather0)

    def gather1(j, s):
        arrive(s.gather0)
        start(s.gather1)

    def gather2(j, s):
        arrive(s.gather1)
        start(s.gather2)

    def gather3(j, s):
        for came, go in zip(s.gather2, s.gather3):
            came.wait_recv()
            go.start()

    def share(j, s):
        arrive(s.gather3)
        s.share.start()

    def finish(j, s):
        s.share.wait_recv()

    STEPS = (exchange, pass_on, mix, sum_q, start_r, activate, gather1, gather2, gather3, share, finish)

    def channel_mix(i):
        gain2, bias2 = g2_ref[...], h2_ref[...]
        shift = b2c[...]
        shift = jnp.concatenate([shift] * 4, axis=1)
        mids = []
        for n in range(ROWS):
            img = i * ROWS + n
            act = gall[img // 8, (img // 4) % 2, img % 4].reshape(256, 512)
            tok = jnp.dot(w2t[...], act, preferred_element_type=F32) + shift
            mids.append((xv[img].astype(F32) + tok).astype(BF16).astype(F32))
        mid = jnp.concatenate(mids, axis=0)
        v = layer_norm(mid, gain2, bias2).astype(BF16)
        total = mid + bc2_ref[...]
        for f in range(0, 2048, 512):
            pre = jnp.dot(v, wc1[:, f:f + 512], preferred_element_type=F32) + bc1_ref[:, f:f + 512]
            total = total + jnp.dot(gelu(pre).astype(BF16), wc2[f:f + 512, :], preferred_element_type=F32)
        xv[pl.ds(i * ROWS, ROWS)] = total.astype(BF16).reshape(ROWS, 128, 512)

    def store(i):
        window = pl.ds(i * ROWS, ROWS)
        return local(xv.at[window], z_hbm.at[window], K + 2)

    start(loads)
    barrier = pltpu.get_barrier_semaphore()
    peers = group + [near[a][s] for a in "yz" for s in (1, 2, 3)]
    for peer in peers:
        pl.semaphore_signal(barrier, inc=1, device_id={"sp": peer}, device_id_type=MESH)
    w1o[...] = w1_ref[...].T
    w2t[...] = w2_ref[...].T
    b2c[...] = jnp.broadcast_to(b2_ref[...], (128, 128)).T
    row = lax.broadcasted_iota(jnp.int32, (16, 128), 0)
    tile_in[8] = jnp.where(row == 2 * slot, b1_ref[0], jnp.where(row == 2 * slot + 1, b1_ref[1], 0.0))
    tile_in[slot] = tile_in[8]
    for i, a in enumerate("xyz"):
        w1t[i, :, lanes(co[a], core)] = w1o[...]
    pl.semaphore_wait(barrier, len(peers))

    norm(0)
    for a in "xyz":
        start(w1_ring[a])
    start([w1_mine[a] for a in "xyz"])
    start(b1_group)
    norm(1)
    for j in (0, 1):
        exchange(j, pieces[j])
    norm(2)
    for j in (2, 3):
        exchange(j, pieces[j])
    norm(3)

    arrive(b1_group)
    tile = tile_in[0]
    for n in range(1, 8):
        tile = tile + tile_in[n]
    tile_all[co["z"], co["y"]] = tile
    start(b1_y)
    for a in "xyz":
        for came, go in zip(w1_ring[a], w1_share[a]):
            came.wait_recv()
            go.start()
    for j in (0, 1):
        pass_on(j, pieces[j])
    arrive(b1_y)
    start(b1_z)
    for a in "xyz":
        arrive([w1_mine[a]] + w1_share[a])
    arrive(b1_z)

    ticks = {}
    for k in range(K):
        for n in range(len(STEPS)):
            ticks.setdefault(n + STEP * k, []).append((n, k))
    first_block = len(STEPS) - 1
    slots = {}
    for t in sorted(ticks):
        todo = [(n, k) for n, k in sorted(ticks[t], key=lambda nk: -nk[0]) if not (n == 0 and k < 2 or n == 1 and k < 1)]

        def run(todo=todo):
            for n, k in todo:
                for j in (2 * k, 2 * k + 1):
                    STEPS[n](j, pieces[j])

        if t <= first_block:
            run()
        else:
            slots.setdefault(((t - first_block) * (8 // ROWS)) // STEP, []).append(run)

    def loop(i, carry):
        for s, runs in slots.items():
            @pl.when(i == s)
            def _():
                for run in runs:
                    run()
        channel_mix(i)
        store(i).start()
        return carry

    loads[K].wait()
    loads[K + 1].wait()
    lax.fori_loop(0, BLOCKS, loop, 0)
    local(xv, z_hbm, K + 2).wait()
    for copy in sent:
        copy.wait_send()


N_COPIES = 27 * N + K + 3 * 7 + 7 + 3 + 3


def vmem(*shape, dtype=BF16):
    return pltpu.VMEM(shape, dtype)


def mixer(x, w1, b1, w2, b2, wc1, bc1, wc2, bc2, g1, h1, g2, h2):
    any_space = pl.BlockSpec(memory_space=pl.ANY)
    whole = pl.BlockSpec(memory_space=pltpu.VMEM)
    scalars = pl.BlockSpec(memory_space=pltpu.SMEM)
    return pl.pallas_call(
        mixer_kernel,
        name="mixer",
        out_shape=jax.ShapeDtypeStruct((32, 128, 512), BF16),
        in_specs=[any_space, whole, scalars, whole, whole, any_space, whole, any_space, whole, whole, whole, whole, whole],
        out_specs=any_space,
        scratch_shapes=[
            vmem(32, 128, 512),
            vmem(256, 128),
            vmem(3, 256, 1024),
            vmem(128, 256),
            vmem(128, 128, dtype=F32),
            vmem(512, 2048),
            vmem(2048, 512),
            vmem(9, 16, 128, dtype=F32),
            vmem(4, 4, 16, 128, dtype=F32),
            vmem(K, 4, 128, 512),
            vmem(K, 4, 2, 128, 512),
            vmem(N, 4, 2, 128, 256),
            vmem(N, 2, 2, 128, 128),
            vmem(N, 4, 4, 16, 256, dtype=F32),
            vmem(N, 2, 4, 16, 128, dtype=F32),
            vmem(N, 2, 4, 16, 128, dtype=F32),
            vmem(N, 2, 4, 16, 128, dtype=F32),
            vmem(N, 4, 16, 256, dtype=F32),
            vmem(N, 4, 16, 256, dtype=F32),
            vmem(K, 2, 4, 4, 4, 16, 512),
            pltpu.SemaphoreType.DMA((N_COPIES,)),
            pltpu.SemaphoreType.DMA((N_COPIES,)),
            pltpu.SemaphoreType.DMA((K + 3,)),
        ],
        compiler_params=pltpu.CompilerParams(
            collective_id=0, has_side_effects=True, vmem_limit_bytes=60 * 1024 * 1024
        ),
    )(
        x, w1, b1, w2, b2.reshape(1, 128), wc1, bc1.reshape(1, 2048), wc2, bc2.reshape(1, 512),
        g1.reshape(1, 512), h1.reshape(1, 512), g2.reshape(1, 512), h2.reshape(1, 512),
    )


def solution(mesh):
    row_spec = P("dp", "sp", None)
    in_specs = (row_spec, P("sp", None), P("sp"), P(None, "sp"), P("sp"), P(None, None), P(None), P(None, None), P(None), P(None), P(None), P(None), P(None))
    return jax.shard_map(mixer, mesh=mesh, in_specs=in_specs, out_specs=row_spec, check_vma=False)
```

```python
import jax
import jax.numpy as jnp
from jax import lax
from jax.experimental import pallas as pl
from jax.experimental.pallas import tpu as pltpu
from jax.sharding import PartitionSpec as P

LN_EPS = 1e-6
F32 = jnp.float32
BF16 = jnp.bfloat16
MESH = pl.DeviceIdType.MESH
PIECES = (
    ("xyz", "zyx"),
    ("zxy", "xyz"),
    ("yxz", "xzy"),
    ("zxy", "zyx"),
    ("yxz", "zxy"),
    ("xyz", "xyz"),
    ("zxy", "zyx"),
    ("yxz", "xzy"),
)
N = len(PIECES)
K = N // 2
NORM, W1_PASS, MLP = 11, 12, 15
ORDER = (
    (11, 1), (11, 2), (0, 0), (0, 1), (11, 3), (0, 2), (1, 2), (12, 0), (1, 1), (0, 3), (0, 4), (1, 0), (0, 5),
    (13, 0), (2, 0), (2, 1), (2, 2), (1, 3), (1, 4), (1, 5), (0, 6), (3, 0), (0, 7), (3, 1), (14, 0), (3, 2),
    (2, 3), (2, 4), (4, 0), (1, 6), (2, 5), (4, 1), (1, 7), (4, 2), (3, 3), (3, 4), (5, 0), (3, 5), (2, 6), (4, 3),
    (5, 2), (5, 1), (4, 4), (2, 7), (6, 0), (4, 5), (3, 6), (5, 3), (6, 2), (6, 1), (5, 4), (3, 7), (5, 5), (4, 6),
    (7, 0), (6, 3), (4, 7), (7, 2), (7, 1), (6, 4), (6, 5), (5, 6), (8, 0), (7, 3), (5, 7), (7, 4), (8, 2), (8, 1),
    (6, 6), (9, 0), (7, 5), (10, 0), (9, 1), (8, 3), (8, 4), (6, 7), (10, 1), (15, 0), (9, 2), (15, 1), (10, 2),
    (9, 3), (8, 5), (15, 2), (10, 3), (9, 4), (7, 6), (7, 7), (15, 3), (10, 4), (15, 4), (9, 5), (15, 5), (10, 5),
    (15, 6), (8, 6), (8, 7), (15, 7), (15, 8), (15, 9), (9, 6), (9, 7), (15, 10), (10, 6), (10, 7), (15, 11),
    (15, 12), (15, 13), (15, 14), (15, 15),
)
ROWS = 2
BLOCKS = 32 // ROWS
C0 = 0.7978845608028654
C1 = C0 * 0.044715


def layer_norm(values, ln_gain, ln_bias):
    mean_val = jnp.mean(values, axis=-1, keepdims=True)
    centred = values - mean_val
    var_val = jnp.mean(centred * centred, axis=-1, keepdims=True)
    return centred * lax.rsqrt(var_val + LN_EPS) * ln_gain + ln_bias


def gelu(a):
    half = 0.5 * a
    return half + half * jnp.tanh(a * (C0 + C1 * (a * a)))


def mixer_kernel(
    x_hbm, w1_ref, b1_ref, w2_ref, b2_ref, wc1_hbm, bc1_ref, wc2_hbm, bc2_ref, g1_ref, h1_ref, g2_ref, h2_ref, z_hbm,
    xv, w1o, w1t, w2t, b2c, wc1, wc2, tile_in, tile_all, usend, ustage, uall, relay, hb, rq, rd, rs, hq, rr, gall, v0, v1, mid0, mid1,
    send_sems, recv_sems, local_sems,
):
    me = lax.axis_index("sp")
    co = {"z": me // 32, "y": (me // 8) % 4, "x": (me // 2) % 4}
    core = me % 2
    other = 1 - core

    def device(c=None, **at):
        z, y, x = (at.get(a, co[a]) for a in "zyx")
        return ((z * 4 + y) * 4 + x) * 2 + (core if c is None else c)

    hop = {a: [co[a]] + [(co[a] + s) % 4 for s in (1, 2, 3)] for a in "xyz"}
    near = {a: [None] + [device(**{a: hop[a][s]}) for s in (1, 2, 3)] for a in "xyz"}
    partner = device(c=other)
    group = [device(c=(core + j) % 2, x=hop["x"][s]) for s in range(4) for j in range(2) if (s, j) != (0, 0)]
    sent = []

    def remote(src, dst, to):
        n = len(sent)
        copy = pltpu.make_async_remote_copy(
            src_ref=src, dst_ref=dst, send_sem=send_sems.at[n], recv_sem=recv_sems.at[n],
            device_id={"sp": to}, device_id_type=MESH,
        )
        sent.append(copy)
        return copy

    def start(copies):
        for copy in copies:
            copy.start()

    def arrive(copies):
        for copy in copies:
            copy.wait_recv()

    def local(src, dst, n):
        return pltpu.make_async_copy(src, dst, local_sems.at[n])

    loads = [local(x_hbm.at[pl.ds(8 * k, 8)], xv.at[pl.ds(8 * k, 8)], k) for k in range(K)]
    loads += [local(wc1_hbm, wc1, K), local(wc2_hbm, wc2, K + 1)]

    def lanes(pos, c):
        return pl.ds(pl.multiple_of((pos * 2 + c) * 128, 128), 128)

    w1_ring, w1_mine, w1_share = {}, {}, {}
    for i, a in enumerate("xyz"):
        dst = w1t.at[i, :, lanes(co[a], core)]
        w1_ring[a] = [remote(w1o, dst, near[a][s]) for s in (1, 2, 3)]
        w1_mine[a] = remote(w1o, dst, partner)
        refs = [w1t.at[i, :, lanes(hop[a][s], core)] for s in (3, 2, 1)]
        w1_share[a] = [remote(ref, ref, partner) for ref in refs]
    slot = co["x"] * 2 + core
    b1_group = [remote(tile_in.at[8], tile_in.at[slot], to) for to in group]
    ref = tile_all.at[co["z"], co["y"]]
    b1_y = [remote(ref, ref, near["y"][s]) for s in (1, 2, 3)]
    ref = tile_all.at[co["z"]]
    b1_z = [remote(ref, ref, near["z"][s]) for s in (1, 2, 3)]
    pairs = [remote(usend.at[k], ustage.at[k, :, core], partner) for k in range(K)]

    class Piece:
        pass

    pieces = []
    for j, (axes, order) in enumerate(PIECES):
        s = Piece()
        s.k, s.h, s.axes, s.order = j // 2, j % 2, axes, order
        a, b, c = axes
        low = s.h * 256
        s.half = half = (pl.ds(low, 128), pl.ds(low + 128, 128))
        s.lanes = pl.ds(low, 256)
        s.at = (co[a], co[c], co[b])
        p, st = hop[a], ustage.at[s.k]
        s.passing = [
            remote(st.at[p[2], :, :, half[0]], relay.at[j, 0], near[a][1]),
            remote(st.at[p[2], :, :, half[1]], relay.at[j, 1], near[a][3]),
        ]
        s.direct = [
            remote(st.at[p[1], :, :, s.lanes], uall.at[j, p[0]], near[a][1]),
            remote(st.at[p[3], :, :, s.lanes], uall.at[j, p[0]], near[a][3]),
        ]
        s.forward = [
            remote(relay.at[j, 0], uall.at[j, p[3], :, :, pl.ds(0, 128)], near[a][1]),
            remote(relay.at[j, 1], uall.at[j, p[1], :, :, pl.ds(128, 128)], near[a][3]),
        ]
        q = hop[b]
        s.part = lambda pos, i, j=j: hb.at[j, :, pos, :, pl.ds(128 * i, 128)]
        s.first = [remote(s.part(q[2], 0), rq.at[j, 0], near[b][1]), remote(s.part(q[2], 1), rq.at[j, 1], near[b][3])]
        s.straight = [remote(s.part(q[1], 1), rd.at[j, 0], near[b][1]), remote(s.part(q[3], 0), rd.at[j, 1], near[b][3])]
        s.second = [remote(s.part(q[1], 0), rs.at[j, 0], near[b][1]), remote(s.part(q[3], 1), rs.at[j, 1], near[b][3])]
        s.last = [remote(hq.at[j, hop[c][d]], rr.at[j, d], near[c][d]) for d in (1, 3, 2)]

        def block(known, axis=None, pos=None, lane=None, s=s):
            names = (s.axes[0], s.axes[2], s.axes[1])
            at = tuple(pos if n == axis else slice(None) if n in known else v for n, v in zip(names, s.at))
            return gall.at[(s.k, core) + at + (slice(None), s.lanes if lane is None else s.half[lane])]

        d0, d1, d2 = order
        own = block("")
        s.gather0 = [remote(own, own, near[d0][d]) for d in (1, 3, 2)]
        own = block(d0)
        s.gather1 = [remote(own, own, near[d1][d]) for d in (1, 3, 2)]
        own = block(d0 + d1)
        s.gather2 = [remote(own, own, near[d2][1]), remote(own, own, near[d2][3])]
        ends = [block(d0 + d1, d2, hop[d2][3], 0), block(d0 + d1, d2, hop[d2][1], 1)]
        s.gather3 = [remote(ends[0], ends[0], near[d2][1]), remote(ends[1], ends[1], near[d2][3])]
        s.share = []
        for d in (0, 1, 3, 2):
            ref = block(d0 + d1, d2, hop[d2][d], None)
            s.share.append(remote(ref, ref, partner))
        pieces.append(s)

    gain1, bias1 = g1_ref[...], h1_ref[...]

    def norm(k):
        loads[k].wait()

        def body(i, carry):
            mine = layer_norm(xv[8 * k + 4 * core + i].astype(F32), gain1, bias1).astype(BF16)
            ustage[k, i, core] = mine
            theirs = layer_norm(xv[8 * k + 4 * other + i].astype(F32), gain1, bias1).astype(BF16)
            usend[k, i] = theirs
            return carry

        lax.fori_loop(0, 4, body, 0)

    def exchange(j, s):
        if s.h == 0:
            pairs[s.k].wait_recv()
        start(s.passing)
        start(s.direct)
        uall[j, s.at[0]] = ustage[s.k, s.at[0], :, :, s.lanes]

    def pass_on(j, s):
        for came, go in zip(s.passing, s.forward):
            came.wait_recv()
            go.start()

    def mix(j, s):
        arrive(s.direct + s.forward)
        u = uall[j].reshape(1024, 256)
        part = jnp.dot(w1t["xyz".index(s.axes[0])], u, preferred_element_type=F32)
        hb[j] = part.reshape(4, 4, 16, 256)
        start(s.first + s.straight)

    def sum_q(j, s):
        q = hop[s.axes[1]]
        for i, pos in enumerate((q[1], q[3])):
            s.first[i].wait_recv()
            ref = s.part(pos, i)
            ref[...] = ref[...] + rq[j, i]
            s.second[i].start()

    def start_r(j, s):
        arrive(s.straight + s.second)
        q = co[s.axes[1]]
        hq[j, :, :, pl.ds(0, 128)] = s.part(q, 0)[...] + rd[j, 1] + rs[j, 0]
        hq[j, :, :, pl.ds(128, 128)] = s.part(q, 1)[...] + rd[j, 0] + rs[j, 1]
        start(s.last)

    def activate(j, s):
        arrive(s.last)
        a, b, c = s.axes
        tile = tile_all[co[c], co[b]]
        total = hq[j, co[c]] + rr[j, 1] + rr[j, 2] + rr[j, 3] + jnp.concatenate([tile, tile], axis=1)
        gall[s.k, core, s.at[0], s.at[1], s.at[2], :, s.lanes] = gelu(total).astype(BF16)
        start(s.gather0)

    def gather1(j, s):
        arrive(s.gather0)
        start(s.gather1)

    def gather2(j, s):
        arrive(s.gather1)
        start(s.gather2)
        s.share[0].start()

    def gather3(j, s):
        for i, (came, go) in enumerate(zip(s.gather2, s.gather3)):
            came.wait_recv()
            go.start()
        start(s.share[1:3])

    def share(j, s):
        arrive(s.gather3)
        s.share[3].start()

    def finish(j, s):
        arrive(s.share)

    STEPS = (exchange, pass_on, mix, sum_q, start_r, activate, gather1, gather2, gather3, share, finish)

    def token_half(i, v_ref, mid_ref):
        shift = jnp.concatenate([b2c[...]] * 4, axis=1)
        for n in range(ROWS):
            img = i * ROWS + n
            act = gall[img // 8, (img // 4) % 2, img % 4].reshape(256, 512)
            tok = jnp.dot(w2t[...], act, preferred_element_type=F32) + shift
            mid = (xv[img].astype(F32) + tok).astype(BF16)
            mid_ref[128 * n:128 * n + 128, :] = mid
            v_ref[128 * n:128 * n + 128, :] = layer_norm(mid.astype(F32), g2_ref[...], h2_ref[...]).astype(BF16)

    def channel_half(i, v_ref, mid_ref):
        total = mid_ref[...].astype(F32) + bc2_ref[...]
        for f in range(0, 2048, 512):
            pre = jnp.dot(v_ref[...], wc1[:, f:f + 512], preferred_element_type=F32) + bc1_ref[:, f:f + 512]
            total = total + jnp.dot(gelu(pre).astype(BF16), wc2[f:f + 512, :], preferred_element_type=F32)
        xv[pl.ds(i * ROWS, ROWS)] = total.astype(BF16).reshape(ROWS, 128, 512)

    def store(i):
        window = pl.ds(i * ROWS, ROWS)
        return local(xv.at[window], z_hbm.at[window], K + 2)

    start(loads)
    barrier = pltpu.get_barrier_semaphore()
    peers = group + [near[a][s] for a in "yz" for s in (1, 2, 3)]
    for peer in peers:
        pl.semaphore_signal(barrier, inc=1, device_id={"sp": peer}, device_id_type=MESH)
    w1o[...] = w1_ref[...].T
    norm(0)
    pl.semaphore_wait(barrier, len(peers))
    pairs[0].start()
    for a in "xyz":
        start(w1_ring[a])
    row = lax.broadcasted_iota(jnp.int32, (16, 128), 0)
    tile_in[8] = jnp.where(row == 2 * slot, b1_ref[0], jnp.where(row == 2 * slot + 1, b1_ref[1], 0.0))
    tile_in[slot] = tile_in[8]
    start(b1_group)
    start([w1_mine[a] for a in "xyz"])
    for i, a in enumerate("xyz"):
        w1t[i, :, lanes(co[a], core)] = w1o[...]
    w2t[...] = w2_ref[...].T
    b2c[...] = jnp.broadcast_to(b2_ref[...], (128, 128)).T

    def later_norm(k):
        norm(k)
        pairs[k].start()

    def w1_pass():
        for a in "xyz":
            for came, go in zip(w1_ring[a], w1_share[a]):
                came.wait_recv()
                go.start()
        arrive(b1_group)
        tile = tile_in[0]
        for n in range(1, 8):
            tile = tile + tile_in[n]
        tile_all[co["z"], co["y"]] = tile
        start(b1_y)

    def w1_end():
        for a in "xyz":
            arrive([w1_mine[a]] + w1_share[a])
        arrive(b1_y)
        start(b1_z)

    def b1_end():
        arrive(b1_z)

    def run(op):
        n, j = op
        if n < len(STEPS):
            STEPS[n](j, pieces[j])
        elif n == NORM:
            later_norm(j)
        else:
            (w1_pass, w1_end, b1_end)[n - W1_PASS]()

    slots, slot_no = {}, 0
    for op in ORDER:
        if op[0] == MLP:
            slot_no = op[1] + 1
        else:
            slots.setdefault(slot_no, []).append(op)
    for op in slots.pop(0, []):
        run(op)
    loads[K].wait()
    loads[K + 1].wait()
    token_half(0, v0, mid0)

    def loop(p, carry):
        for side, (mine, ahead) in enumerate((((v0, mid0), (v1, mid1)), ((v1, mid1), (v0, mid0)))):
            i = 2 * p + side
            for s, ops in slots.items():
                if s % 2 == side:
                    @pl.when(p == s // 2)
                    def _():
                        for op in ops:
                            run(op)
            token_half(jnp.minimum(i + 1, BLOCKS - 1), *ahead)
            channel_half(i, *mine)
            store(i).start()
        return carry

    lax.fori_loop(0, BLOCKS // 2, loop, 0)
    local(xv, z_hbm, K + 2).wait()
    for copy in sent:
        copy.wait_send()


N_COPIES = 30 * N + K + 3 * 7 + 7 + 3 + 3


def vmem(*shape, dtype=BF16):
    return pltpu.VMEM(shape, dtype)


def mixer(x, w1, b1, w2, b2, wc1, bc1, wc2, bc2, g1, h1, g2, h2):
    any_space = pl.BlockSpec(memory_space=pl.ANY)
    whole = pl.BlockSpec(memory_space=pltpu.VMEM)
    scalars = pl.BlockSpec(memory_space=pltpu.SMEM)
    return pl.pallas_call(
        mixer_kernel,
        name="mixer",
        out_shape=jax.ShapeDtypeStruct((32, 128, 512), BF16),
        in_specs=[any_space, whole, scalars, whole, whole, any_space, whole, any_space, whole, whole, whole, whole, whole],
        out_specs=any_space,
        scratch_shapes=[
            vmem(32, 128, 512),
            vmem(256, 128),
            vmem(3, 256, 1024),
            vmem(128, 256),
            vmem(128, 128, dtype=F32),
            vmem(512, 2048),
            vmem(2048, 512),
            vmem(9, 16, 128, dtype=F32),
            vmem(4, 4, 16, 128, dtype=F32),
            vmem(K, 4, 128, 512),
            vmem(K, 4, 2, 128, 512),
            vmem(N, 4, 2, 128, 256),
            vmem(N, 2, 2, 128, 128),
            vmem(N, 4, 4, 16, 256, dtype=F32),
            vmem(N, 2, 4, 16, 128, dtype=F32),
            vmem(N, 2, 4, 16, 128, dtype=F32),
            vmem(N, 2, 4, 16, 128, dtype=F32),
            vmem(N, 4, 16, 256, dtype=F32),
            vmem(N, 4, 16, 256, dtype=F32),
            vmem(K, 2, 4, 4, 4, 16, 512),
            vmem(128 * ROWS, 512),
            vmem(128 * ROWS, 512),
            vmem(128 * ROWS, 512),
            vmem(128 * ROWS, 512),
            pltpu.SemaphoreType.DMA((N_COPIES,)),
            pltpu.SemaphoreType.DMA((N_COPIES,)),
            pltpu.SemaphoreType.DMA((K + 3,)),
        ],
        compiler_params=pltpu.CompilerParams(
            collective_id=0, has_side_effects=True, vmem_limit_bytes=60 * 1024 * 1024
        ),
    )(
        x, w1, b1, w2, b2.reshape(1, 128), wc1, bc1.reshape(1, 2048), wc2, bc2.reshape(1, 512),
        g1.reshape(1, 512), h1.reshape(1, 512), g2.reshape(1, 512), h2.reshape(1, 512),
    )


def solution(mesh):
    row_spec = P("dp", "sp", None)
    in_specs = (row_spec, P("sp", None), P("sp"), P(None, "sp"), P("sp"), P(None, None), P(None), P(None, None), P(None), P(None), P(None), P(None), P(None))
    return jax.shard_map(mixer, mesh=mesh, in_specs=in_specs, out_specs=row_spec, check_vma=False)
```

```python
import jax
import jax.numpy as jnp
from jax import lax
from jax.experimental import pallas as pl
from jax.experimental.pallas import tpu as pltpu
from jax.sharding import PartitionSpec as P

LN_EPS = 1e-6
F32 = jnp.float32
BF16 = jnp.bfloat16
MESH = pl.DeviceIdType.MESH
PIECES = (
    ("zyx", "xyz"),
    ("yzx", "xzy"),
    ("zxy", "zyx"),
    ("xyz", "zxy"),
    ("yzx", "yxz"),
    ("xzy", "yxz"),
    ("xzy", "zxy"),
    ("yxz", "xzy"),
)
N = len(PIECES)
NORM, W1_PASS = 11, 12
ORDER = (
    (111, 112, 0, 113, 114, 115, 1, 2, 116, 3, 117, 5, 11, 120, 10, 13, 4, 12, 130, 21, 15, 14, 6, 20, 23, 22, 24,
     25, 140, 30, 16, 7, 31, 33, 34, 40, 35, 32, 17, 41, 44, 26, 45, 50, 42, 43, 51, 36, 27, 54, 60, 55, 52, 53,
     61, 46, 37, 64, 70, 62, 63, 65, 47, 56, 71, 74, 72, 73, 80, 57, 66, 75, 81, 84, 82, 83, 90, 67, 91, 100,),
    (101, 76,),
    (92, 93, 85,),
    (102, 103, 94,),
    (104, 77,),
    (95, 86,),
    (105,),
    (),
    (87,),
    (96,),
    (106,),
    (97,),
    (107,),
    (),
    (),
    (),
)
BLOCKS = 2 * N
C0 = 0.7978845608028654
C1 = C0 * 0.044715


def layer_norm(values, ln_gain, ln_bias):
    mean_val = jnp.mean(values, axis=-1, keepdims=True)
    centred = values - mean_val
    var_val = jnp.mean(centred * centred, axis=-1, keepdims=True)
    return centred * lax.rsqrt(var_val + LN_EPS) * ln_gain + ln_bias


def gelu_of_half(h):
    return h + h * jnp.tanh(h * (2.0 * C0 + (8.0 * C1) * (h * h)))


def mixer_kernel(
    x_hbm, w1_hbm, b1_ref, w2_hbm, vec_hbm, wc1_hbm, bc1_hbm, wc2_hbm, z_hbm,
    xv, w1v, w2v, vec, bc1, w1o, w1t, w2t, b2c, wc1, wc2, tile_in, tile_all, usend, ustage, uall, relay,
    hb, rq, rd, rs, hq, rr, gall, va, vb, mida, midb, prea, preb, acta, actb, acc,
    send_sems, recv_sems, local_sems,
):
    me = lax.axis_index("sp")
    co = {"z": me // 32, "y": (me // 8) % 4, "x": (me // 2) % 4}
    core = me % 2
    other = 1 - core

    def device(c=None, **at):
        z, y, x = (at.get(a, co[a]) for a in "zyx")
        return ((z * 4 + y) * 4 + x) * 2 + (core if c is None else c)

    hop = {a: [co[a]] + [(co[a] + s) % 4 for s in (1, 2, 3)] for a in "xyz"}
    near = {a: [None] + [device(**{a: hop[a][s]}) for s in (1, 2, 3)] for a in "xyz"}
    partner = device(c=other)
    group = [device(c=(core + j) % 2, x=hop["x"][s]) for s in range(4) for j in range(2) if (s, j) != (0, 0)]
    sent = []

    def remote(src, dst, to):
        n = len(sent)
        copy = pltpu.make_async_remote_copy(
            src_ref=src, dst_ref=dst, send_sem=send_sems.at[n], recv_sem=recv_sems.at[n],
            device_id={"sp": to}, device_id_type=MESH,
        )
        sent.append(copy)
        return copy

    def start(copies):
        for copy in copies:
            copy.start()

    def arrive(copies):
        for copy in copies:
            copy.wait_recv()

    def local(src, dst, n):
        return pltpu.make_async_copy(src, dst, local_sems.at[n])

    loads = [local(x_hbm.at[pl.ds(4 * j, 4)], xv.at[pl.ds(4 * j, 4)], j) for j in range(N)]
    small = [local(vec_hbm, vec, N), local(w1_hbm, w1v, N + 1), local(w2_hbm, w2v, N + 2), local(bc1_hbm, bc1, N + 3)]
    large = [local(wc1_hbm, wc1, N + 4), local(wc2_hbm, wc2, N + 5)]

    def lanes(pos, c):
        return pl.ds(pl.multiple_of((pos * 2 + c) * 128, 128), 128)

    rings = sorted({axes[0] for axes, _ in PIECES})
    w1_ring, w1_mine, w1_share = {}, {}, {}
    for i, a in enumerate(rings):
        dst = w1t.at[i, :, lanes(co[a], core)]
        w1_ring[a] = [remote(w1o, dst, near[a][s]) for s in (1, 2, 3)]
        w1_mine[a] = remote(w1o, dst, partner)
        refs = [w1t.at[i, :, lanes(hop[a][s], core)] for s in (3, 2, 1)]
        w1_share[a] = [remote(ref, ref, partner) for ref in refs]
    slot = co["x"] * 2 + core
    b1_group = [remote(tile_in.at[8], tile_in.at[slot], to) for to in group]
    ref = tile_all.at[co["z"], co["y"]]
    b1_y = [remote(ref, ref, near["y"][s]) for s in (1, 2, 3)]
    ref = tile_all.at[co["z"]]
    b1_z = [remote(ref, ref, near["z"][s]) for s in (1, 2, 3)]

    class Piece:
        pass

    low, high = pl.ds(0, 128), pl.ds(128, 128)
    half = (low, high)
    pieces = []
    for j, (axes, order) in enumerate(PIECES):
        s = Piece()
        s.axes = axes
        a, b, c = axes
        s.at = (co[a], co[c], co[b])
        s.pair = remote(usend.at[j], ustage.at[j, :, core], partner)
        p, st = hop[a], ustage.at[j]
        s.passing = [
            remote(st.at[p[2], :, :, low], relay.at[j, 0], near[a][1]),
            remote(st.at[p[2], :, :, high], relay.at[j, 1], near[a][3]),
        ]
        s.direct = [
            remote(st.at[p[1]], uall.at[j, p[0]], near[a][1]),
            remote(st.at[p[3]], uall.at[j, p[0]], near[a][3]),
        ]
        s.forward = [
            remote(relay.at[j, 0], uall.at[j, p[3], :, :, low], near[a][1]),
            remote(relay.at[j, 1], uall.at[j, p[1], :, :, high], near[a][3]),
        ]
        q = hop[b]
        s.part = lambda pos, i, j=j: hb.at[j, :, pos, :, half[i]]
        s.first = [remote(s.part(q[2], 0), rq.at[j, 0], near[b][1]), remote(s.part(q[2], 1), rq.at[j, 1], near[b][3])]
        s.straight = [remote(s.part(q[1], 1), rd.at[j, 0], near[b][1]), remote(s.part(q[3], 0), rd.at[j, 1], near[b][3])]
        s.second = [remote(s.part(q[1], 0), rs.at[j, 0], near[b][1]), remote(s.part(q[3], 1), rs.at[j, 1], near[b][3])]
        s.last = [remote(hq.at[j, hop[c][d]], rr.at[j, d], near[c][d]) for d in (1, 3, 2)]

        def block(known, axis=None, pos=None, lane=slice(None), s=s, j=j):
            names = (s.axes[0], s.axes[2], s.axes[1])
            at = tuple(pos if n == axis else slice(None) if n in known else v for n, v in zip(names, s.at))
            return gall.at[(j, core) + at + (slice(None), lane)]

        d0, d1, d2 = order
        own = block("")
        s.gather0 = [remote(own, own, near[d0][d]) for d in (1, 3, 2)]
        own = block(d0)
        s.gather1 = [remote(own, own, near[d1][d]) for d in (1, 3, 2)]
        own = block(d0 + d1)
        s.gather2 = [remote(own, own, near[d2][1]), remote(own, own, near[d2][3])]
        ends = [block(d0 + d1, d2, hop[d2][3], low), block(d0 + d1, d2, hop[d2][1], high)]
        s.gather3 = [remote(ends[0], ends[0], near[d2][1]), remote(ends[1], ends[1], near[d2][3])]
        s.share = []
        for d in (0, 1, 3, 2):
            ref = block(d0 + d1, d2, hop[d2][d])
            s.share.append(remote(ref, ref, partner))
        pieces.append(s)

    def norm(j):
        loads[j].wait()
        gain1, bias1 = vec[0:1, :], vec[1:2, :]
        for n in range(2):
            mine = layer_norm(xv[4 * j + 2 * core + n].astype(F32), gain1, bias1).astype(BF16)
            ustage[j, 2 * n, core] = mine[:, :256]
            ustage[j, 2 * n + 1, core] = mine[:, 256:]
            theirs = layer_norm(xv[4 * j + 2 * other + n].astype(F32), gain1, bias1).astype(BF16)
            usend[j, 2 * n] = theirs[:, :256]
            usend[j, 2 * n + 1] = theirs[:, 256:]

    def exchange(j, s):
        s.pair.wait_recv()
        start(s.passing)
        start(s.direct)
        uall[j, s.at[0]] = ustage[j, s.at[0]]

    def pass_on(j, s):
        for came, go in zip(s.passing, s.forward):
            came.wait_recv()
            go.start()

    def mix(j, s):
        arrive(s.direct + s.forward)
        u = uall[j].reshape(1024, 256)
        part = jnp.dot(w1t[rings.index(s.axes[0])], u, preferred_element_type=F32)
        hb[j] = part.reshape(4, 4, 16, 256)
        start(s.first + s.straight)

    def sum_q(j, s):
        q = hop[s.axes[1]]
        for i, pos in enumerate((q[1], q[3])):
            s.first[i].wait_recv()
            ref = s.part(pos, i)
            ref[...] = ref[...] + rq[j, i]
            s.second[i].start()

    def start_r(j, s):
        arrive(s.straight + s.second)
        q = co[s.axes[1]]
        hq[j, :, :, low] = s.part(q, 0)[...] + rd[j, 1] + rs[j, 0]
        hq[j, :, :, high] = s.part(q, 1)[...] + rd[j, 0] + rs[j, 1]
        start(s.last)

    def activate(j, s):
        arrive(s.last)
        a, b, c = s.axes
        tile = tile_all[co[c], co[b]]
        total = hq[j, co[c]] + rr[j, 1] + rr[j, 2] + rr[j, 3] + jnp.concatenate([tile, tile], axis=1)
        gall[j, core, s.at[0], s.at[1], s.at[2]] = gelu_of_half(0.5 * total).astype(BF16)
        start(s.gather0)

    def gather1(j, s):
        arrive(s.gather0)
        start(s.gather1)

    def gather2(j, s):
        arrive(s.gather1)
        start(s.gather2)
        s.share[0].start()

    def gather3(j, s):
        for came, go in zip(s.gather2, s.gather3):
            came.wait_recv()
            go.start()
        start(s.share[1:3])

    def share(j, s):
        arrive(s.gather3)
        s.share[3].start()

    def finish(j, s):
        arrive(s.share)

    STEPS = (exchange, pass_on, mix, sum_q, start_r, activate, gather1, gather2, gather3, share, finish)

    def token_half(i, v_ref, mid_ref):
        shift = jnp.concatenate([b2c[...]] * 2, axis=1)
        gain2, bias2 = 0.5 * vec[2:3, :], 0.5 * vec[3:4, :]
        for n in range(2):
            toks = []
            for h in range(2):
                act = gall[i // 2, i % 2, 2 * n + h].reshape(256, 256)
                toks.append(jnp.dot(w2t[...], act, preferred_element_type=F32) + shift)
            mid = (xv[2 * i + n].astype(F32) + jnp.concatenate(toks, axis=1)).astype(BF16)
            mid_ref[128 * n:128 * n + 128, :] = mid
            v_ref[128 * n:128 * n + 128, :] = layer_norm(mid.astype(F32), gain2, bias2).astype(BF16)

    def widen(f, v_ref, pre_ref):
        pre_ref[...] = jnp.dot(v_ref[...], wc1[:, 512 * f:512 * f + 512], preferred_element_type=F32)

    def bend(f, pre_ref, act_ref):
        act_ref[...] = gelu_of_half(pre_ref[...] + 0.5 * bc1[:, 512 * f:512 * f + 512]).astype(BF16)

    def narrow(f, act_ref):
        return jnp.dot(act_ref[...], wc2[512 * f:512 * f + 512, :], preferred_element_type=F32)

    def store(i):
        window = pl.ds(2 * i, 2)
        return local(xv.at[window], z_hbm.at[window], N + 6)

    def end_block(i, mid_ref):
        total = mid_ref[...].astype(F32) + vec[4:5, :] + acc[...] + narrow(3, actb)
        xv[pl.ds(2 * i, 2)] = total.astype(BF16).reshape(2, 128, 512)

    def channel_mix(i, mine, ahead):
        (v_ref, mid_ref), (v_next, mid_next) = mine, ahead
        token_half(jnp.minimum(i + 1, BLOCKS - 1), v_next, mid_next)
        widen(1, v_ref, preb)
        bend(0, prea, acta)
        widen(2, v_ref, prea)
        acc[...] = narrow(0, acta)
        bend(1, preb, actb)
        widen(3, v_ref, preb)
        acc[...] += narrow(1, actb)
        bend(2, prea, acta)
        widen(0, v_next, prea)
        acc[...] += narrow(2, acta)
        bend(3, preb, actb)
        end_block(i, mid_ref)
        store(i).start()

    barrier = pltpu.get_barrier_semaphore()
    peers = group + [near[a][s] for a in "yz" for s in (1, 2, 3)]
    for peer in peers:
        pl.semaphore_signal(barrier, inc=1, device_id={"sp": peer}, device_id_type=MESH)
    start([small[0], loads[0], small[1]])
    start(loads[1:])
    start(small[2:] + large)
    small[0].wait()
    norm(0)
    small[1].wait()
    w1o[...] = w1v[...].T
    pl.semaphore_wait(barrier, len(peers))
    pieces[0].pair.start()
    for a in rings:
        start(w1_ring[a])
    row = lax.broadcasted_iota(jnp.int32, (16, 128), 0)
    tile_in[8] = jnp.where(row == 2 * slot, b1_ref[0], jnp.where(row == 2 * slot + 1, b1_ref[1], 0.0))
    tile_in[slot] = tile_in[8]
    start(b1_group)
    start([w1_mine[a] for a in rings])
    for i, a in enumerate(rings):
        w1t[i, :, lanes(co[a], core)] = w1o[...]
    small[2].wait()
    w2t[...] = w2v[...].T
    b2c[...] = jnp.broadcast_to(vec[5:6, 0:128], (128, 128)).T

    def later_norm(j):
        norm(j)
        pieces[j].pair.start()

    def w1_pass():
        for a in rings:
            for came, go in zip(w1_ring[a], w1_share[a]):
                came.wait_recv()
                go.start()
        arrive(b1_group)
        tile = tile_in[0]
        for n in range(1, 8):
            tile = tile + tile_in[n]
        tile_all[co["z"], co["y"]] = tile
        start(b1_y)

    def w1_end():
        for a in rings:
            arrive([w1_mine[a]] + w1_share[a])
        arrive(b1_y)
        start(b1_z)

    def b1_end():
        arrive(b1_z)

    def run(code):
        n, j = code // 10, code % 10
        if n < len(STEPS):
            STEPS[n](j, pieces[j])
        elif n == NORM:
            later_norm(j)
        else:
            (w1_pass, w1_end, b1_end)[n - W1_PASS]()

    slots = {n: ops for n, ops in enumerate(ORDER) if ops}
    for code in slots.pop(0, ()):
        run(code)
    small[3].wait()
    for load in large:
        load.wait()
    token_half(0, va, mida)
    widen(0, va, prea)

    def loop(p, carry):
        for side, (mine, ahead) in enumerate((((va, mida), (vb, midb)), ((vb, midb), (va, mida)))):
            for n, ops in slots.items():
                if n % 2 == 1 - side:
                    @pl.when(p == (n - 1) // 2)
                    def _():
                        for code in ops:
                            run(code)
            channel_mix(2 * p + side, mine, ahead)
        return carry

    lax.fori_loop(0, BLOCKS // 2, loop, 0)
    local(xv, z_hbm, N + 6).wait()
    for copy in sent:
        copy.wait_send()


RINGS = len({axes[0] for axes, _ in PIECES})
N_COPIES = 31 * N + 7 * RINGS + 7 + 3 + 3


def vmem(*shape, dtype=BF16):
    return pltpu.VMEM(shape, dtype)


def mixer(x, w1, b1, w2, b2, wc1, bc1, wc2, bc2, g1, h1, g2, h2):
    any_space = pl.BlockSpec(memory_space=pl.ANY)
    scalars = pl.BlockSpec(memory_space=pltpu.SMEM)
    rows = [g1, h1, g2, h2, bc2, jnp.pad(b2, (0, 384))]
    return pl.pallas_call(
        mixer_kernel,
        name="mixer",
        out_shape=jax.ShapeDtypeStruct((32, 128, 512), BF16),
        in_specs=[any_space, any_space, scalars] + [any_space] * 5,
        out_specs=any_space,
        scratch_shapes=[
            vmem(32, 128, 512),
            vmem(128, 256),
            vmem(256, 128),
            vmem(8, 512, dtype=F32),
            vmem(1, 2048, dtype=F32),
            vmem(256, 128),
            vmem(RINGS, 256, 1024),
            vmem(128, 256),
            vmem(128, 128, dtype=F32),
            vmem(512, 2048),
            vmem(2048, 512),
            vmem(9, 16, 128, dtype=F32),
            vmem(4, 4, 16, 128, dtype=F32),
            vmem(N, 4, 128, 256),
            vmem(N, 4, 2, 128, 256),
            vmem(N, 4, 2, 128, 256),
            vmem(N, 2, 2, 128, 128),
            vmem(N, 4, 4, 16, 256, dtype=F32),
            vmem(N, 2, 4, 16, 128, dtype=F32),
            vmem(N, 2, 4, 16, 128, dtype=F32),
            vmem(N, 2, 4, 16, 128, dtype=F32),
            vmem(N, 4, 16, 256, dtype=F32),
            vmem(N, 4, 16, 256, dtype=F32),
            vmem(N, 2, 4, 4, 4, 16, 256),
            vmem(256, 512),
            vmem(256, 512),
            vmem(256, 512),
            vmem(256, 512),
            vmem(256, 512, dtype=F32),
            vmem(256, 512, dtype=F32),
            vmem(256, 512),
            vmem(256, 512),
            vmem(256, 512, dtype=F32),
            pltpu.SemaphoreType.DMA((N_COPIES,)),
            pltpu.SemaphoreType.DMA((N_COPIES,)),
            pltpu.SemaphoreType.DMA((N + 7,)),
        ],
        compiler_params=pltpu.CompilerParams(
            collective_id=0, has_side_effects=True, vmem_limit_bytes=60 * 1024 * 1024
        ),
    )(x, w1, b1, w2, jnp.pad(jnp.stack(rows), ((0, 2), (0, 0))), wc1, bc1.reshape(1, 2048), wc2)


def solution(mesh):
    row_spec = P("dp", "sp", None)
    in_specs = (row_spec, P("sp", None), P("sp"), P(None, "sp"), P("sp"), P(None, None), P(None), P(None, None), P(None), P(None), P(None), P(None), P(None))
    return jax.shard_map(mixer, mesh=mesh, in_specs=in_specs, out_specs=row_spec, check_vma=False)
```

```python
import jax
import jax.numpy as jnp
from jax import lax
from jax.experimental import pallas as pl
from jax.experimental.pallas import tpu as pltpu
from jax.sharding import PartitionSpec as P

LN_EPS = 1e-6
F32 = jnp.float32
BF16 = jnp.bfloat16
MESH = pl.DeviceIdType.MESH
PIECES = (
    ("zxy", "xzy"),
    ("yzx", "zyx"),
    ("xzy", "zxy"),
    ("xyz", "yxz"),
    ("yzx", "xzy"),
    ("zxy", "yxz"),
    ("yzx", "xzy"),
    ("xyz", "zxy"),
)
N = len(PIECES)
NAMES = "abcdefghijk"
ORDER = (
    ("n1n2a0n3n4n5a1a2n6a3n7w0b0b1b2a4a5a6v0c0c1b3b5b4", "c2d0b6a7u0d1c3c5e0d2c4b7e1c6d3e2d4d5f0d6e3c7f2e4",
     "f1e5e6g0d7f3g2g1f4f5f6e7h0g3h2h1g4g5g6f7h3i0h4i1", "i2h6j0g7h5k0",
    ),
    "j1i3i4k1", "j2h7", "k2i5", "j3i6", "k3", "j4", "k4j5", "k5i7", "j6", "k6", "", "j7", "k7",
)
BLOCKS = 2 * N
C0 = 0.7978845608028654
C1 = C0 * 0.044715


def layer_norm(values, ln_gain, ln_bias):
    mean_val = jnp.mean(values, axis=-1, keepdims=True)
    centred = values - mean_val
    var_val = jnp.mean(centred * centred, axis=-1, keepdims=True)
    return centred * lax.rsqrt(var_val + LN_EPS) * ln_gain + ln_bias


def gelu_of_half(h):
    return h + h * jnp.tanh(h * (2.0 * C0 + (8.0 * C1) * (h * h)))


def mixer_kernel(
    x_hbm, w1_hbm, b1_ref, w2_hbm, b2_hbm, wc1_hbm, bc1_hbm, wc2_hbm, bc2_hbm, g1_hbm, h1_hbm, g2_hbm, h2_hbm, z_hbm,
    xv, w1v, w2v, g1, h1, g2, h2, bc2, b2, bc1, w1o, w1t, w2t, b2c, wc1, wc2, tile_in, tile_all, usend, ustage, uall, relay,
    hb, rq, rd, rs, hq, rr, gall, va, vb, mida, midb, prea, preb, acta, actb, acc,
    send_sems, recv_sems, local_sems,
):
    me = lax.axis_index("sp")
    co = {"z": me // 32, "y": (me // 8) % 4, "x": (me // 2) % 4}
    core = me % 2
    other = 1 - core

    def device(c=None, **at):
        z, y, x = (at.get(a, co[a]) for a in "zyx")
        return ((z * 4 + y) * 4 + x) * 2 + (core if c is None else c)

    hop = {a: [co[a]] + [(co[a] + s) % 4 for s in (1, 2, 3)] for a in "xyz"}
    near = {a: [None] + [device(**{a: hop[a][s]}) for s in (1, 2, 3)] for a in "xyz"}
    partner = device(c=other)
    group = [device(c=(core + j) % 2, x=hop["x"][s]) for s in range(4) for j in range(2) if (s, j) != (0, 0)]
    sent = []

    def remote(src, dst, to):
        n = len(sent)
        copy = pltpu.make_async_remote_copy(
            src_ref=src, dst_ref=dst, send_sem=send_sems.at[n], recv_sem=recv_sems.at[n],
            device_id={"sp": to}, device_id_type=MESH,
        )
        sent.append(copy)
        return copy

    def start(copies):
        for copy in copies:
            copy.start()

    def arrive(copies):
        for copy in copies:
            copy.wait_recv()

    def local(src, dst, n):
        return pltpu.make_async_copy(src, dst, local_sems.at[n])

    loads = [local(x_hbm.at[pl.ds(4 * j, 4)], xv.at[pl.ds(4 * j, 4)], j) for j in range(N)]
    early = [local(src, dst, N + n) for n, (src, dst) in enumerate(((g1_hbm, g1), (h1_hbm, h1), (w1_hbm, w1v)))]
    middle = [local(src, dst, N + 3 + n) for n, (src, dst) in enumerate(((w2_hbm, w2v), (b2_hbm, b2)))]
    late = ((g2_hbm, g2), (h2_hbm, h2), (bc1_hbm, bc1), (bc2_hbm, bc2), (wc1_hbm, wc1), (wc2_hbm, wc2))
    late = [local(src, dst, N + 5 + n) for n, (src, dst) in enumerate(late)]
    out_sem = N + 5 + len(late)

    def lanes(pos, c):
        return pl.ds(pl.multiple_of((pos * 2 + c) * 128, 128), 128)

    rings = sorted({axes[0] for axes, _ in PIECES})
    w1_ring, w1_mine, w1_share = {}, {}, {}
    for i, a in enumerate(rings):
        dst = w1t.at[i, :, lanes(co[a], core)]
        w1_ring[a] = [remote(w1o, dst, near[a][s]) for s in (1, 2, 3)]
        w1_mine[a] = remote(w1o, dst, partner)
        refs = [w1t.at[i, :, lanes(hop[a][s], core)] for s in (3, 2, 1)]
        w1_share[a] = [remote(ref, ref, partner) for ref in refs]
    slot = co["x"] * 2 + core
    b1_group = [remote(tile_in.at[8], tile_in.at[slot], to) for to in group]
    ref = tile_all.at[co["z"], co["y"]]
    b1_y = [remote(ref, ref, near["y"][s]) for s in (1, 2, 3)]
    ref = tile_all.at[co["z"]]
    b1_z = [remote(ref, ref, near["z"][s]) for s in (1, 2, 3)]

    class Piece:
        pass

    low, high = pl.ds(0, 128), pl.ds(128, 128)
    half = (low, high)
    pieces = []
    for j, (axes, order) in enumerate(PIECES):
        s = Piece()
        s.axes = axes
        a, b, c = axes
        s.at = (co[a], co[c], co[b])
        s.pair = remote(usend.at[j], ustage.at[j, :, core], partner)
        p, st = hop[a], ustage.at[j]
        s.passing = [
            remote(st.at[p[2], :, :, low], relay.at[j, 0], near[a][1]),
            remote(st.at[p[2], :, :, high], relay.at[j, 1], near[a][3]),
        ]
        s.direct = [
            remote(st.at[p[1]], uall.at[j, p[0]], near[a][1]),
            remote(st.at[p[3]], uall.at[j, p[0]], near[a][3]),
        ]
        s.forward = [
            remote(relay.at[j, 0], uall.at[j, p[3], :, :, low], near[a][1]),
            remote(relay.at[j, 1], uall.at[j, p[1], :, :, high], near[a][3]),
        ]
        q = hop[b]
        s.part = lambda pos, i, j=j: hb.at[j, :, pos, :, half[i]]
        s.first = [remote(s.part(q[2], 0), rq.at[j, 0], near[b][1]), remote(s.part(q[2], 1), rq.at[j, 1], near[b][3])]
        s.straight = [remote(s.part(q[1], 1), rd.at[j, 0], near[b][1]), remote(s.part(q[3], 0), rd.at[j, 1], near[b][3])]
        s.second = [remote(s.part(q[1], 0), rs.at[j, 0], near[b][1]), remote(s.part(q[3], 1), rs.at[j, 1], near[b][3])]
        s.last = [remote(hq.at[j, hop[c][d]], rr.at[j, d], near[c][d]) for d in (1, 3, 2)]

        def block(known, axis=None, pos=None, lane=slice(None), s=s, j=j):
            names = (s.axes[0], s.axes[2], s.axes[1])
            at = tuple(pos if n == axis else slice(None) if n in known else v for n, v in zip(names, s.at))
            return gall.at[(j, core) + at + (slice(None), lane)]

        d0, d1, d2 = order
        own = block("")
        s.gather0 = [remote(own, own, near[d0][d]) for d in (1, 3, 2)]
        own = block(d0)
        s.gather1 = [remote(own, own, near[d1][d]) for d in (1, 3, 2)]
        own = block(d0 + d1)
        s.gather2 = [remote(own, own, near[d2][1]), remote(own, own, near[d2][3])]
        ends = [block(d0 + d1, d2, hop[d2][3], low), block(d0 + d1, d2, hop[d2][1], high)]
        s.gather3 = [remote(ends[0], ends[0], near[d2][1]), remote(ends[1], ends[1], near[d2][3])]
        s.share = []
        for d in (0, 1, 3, 2):
            ref = block(d0 + d1, d2, hop[d2][d])
            s.share.append(remote(ref, ref, partner))
        pieces.append(s)

    def norm(j):
        loads[j].wait()
        gain1, bias1 = g1[...], h1[...]
        for n in range(2):
            mine = layer_norm(xv[4 * j + 2 * core + n].astype(F32), gain1, bias1).astype(BF16)
            ustage[j, 2 * n, core] = mine[:, :256]
            ustage[j, 2 * n + 1, core] = mine[:, 256:]
            theirs = layer_norm(xv[4 * j + 2 * other + n].astype(F32), gain1, bias1).astype(BF16)
            usend[j, 2 * n] = theirs[:, :256]
            usend[j, 2 * n + 1] = theirs[:, 256:]

    def exchange(j, s):
        s.pair.wait_recv()
        start(s.passing)
        start(s.direct)
        uall[j, s.at[0]] = ustage[j, s.at[0]]

    def pass_on(j, s):
        for came, go in zip(s.passing, s.forward):
            came.wait_recv()
            go.start()

    def mix(j, s):
        arrive(s.direct + s.forward)
        u = uall[j].reshape(1024, 256)
        part = jnp.dot(w1t[rings.index(s.axes[0])], u, preferred_element_type=F32)
        hb[j] = part.reshape(4, 4, 16, 256)
        start(s.first + s.straight)

    def sum_q(j, s):
        q = hop[s.axes[1]]
        for i, pos in enumerate((q[1], q[3])):
            s.first[i].wait_recv()
            ref = s.part(pos, i)
            ref[...] = ref[...] + rq[j, i]
            s.second[i].start()

    def start_r(j, s):
        arrive(s.straight + s.second)
        q = co[s.axes[1]]
        hq[j, :, :, low] = s.part(q, 0)[...] + rd[j, 1] + rs[j, 0]
        hq[j, :, :, high] = s.part(q, 1)[...] + rd[j, 0] + rs[j, 1]
        start(s.last)

    def activate(j, s):
        arrive(s.last)
        a, b, c = s.axes
        tile = tile_all[co[c], co[b]]
        total = hq[j, co[c]] + rr[j, 1] + rr[j, 2] + rr[j, 3] + jnp.concatenate([tile, tile], axis=1)
        gall[j, core, s.at[0], s.at[1], s.at[2]] = gelu_of_half(0.5 * total).astype(BF16)
        start(s.gather0)

    def gather1(j, s):
        arrive(s.gather0)
        start(s.gather1)

    def gather2(j, s):
        arrive(s.gather1)
        start(s.gather2)
        s.share[0].start()

    def gather3(j, s):
        for came, go in zip(s.gather2, s.gather3):
            came.wait_recv()
            go.start()
        start(s.share[1:3])

    def share(j, s):
        arrive(s.gather3)
        s.share[3].start()

    def finish(j, s):
        arrive(s.share)

    STEPS = (exchange, pass_on, mix, sum_q, start_r, activate, gather1, gather2, gather3, share, finish)

    def token_half(i, v_ref, mid_ref):
        shift = jnp.concatenate([b2c[...]] * 2, axis=1)
        gain2, bias2 = 0.5 * g2[...], 0.5 * h2[...]
        for n in range(2):
            toks = []
            for h in range(2):
                act = gall[i // 2, i % 2, 2 * n + h].reshape(256, 256)
                toks.append(jnp.dot(w2t[...], act, preferred_element_type=F32) + shift)
            mid = (xv[2 * i + n].astype(F32) + jnp.concatenate(toks, axis=1)).astype(BF16)
            mid_ref[128 * n:128 * n + 128, :] = mid
            v_ref[128 * n:128 * n + 128, :] = layer_norm(mid.astype(F32), gain2, bias2).astype(BF16)

    def widen(f, v_ref, pre_ref):
        pre_ref[...] = jnp.dot(v_ref[...], wc1[:, 512 * f:512 * f + 512], preferred_element_type=F32)

    def bend(f, pre_ref, act_ref):
        act_ref[...] = gelu_of_half(pre_ref[...] + 0.5 * bc1[:, 512 * f:512 * f + 512]).astype(BF16)

    def narrow(f, act_ref):
        return jnp.dot(act_ref[...], wc2[512 * f:512 * f + 512, :], preferred_element_type=F32)

    def store(i):
        window = pl.ds(2 * i, 2)
        return local(xv.at[window], z_hbm.at[window], out_sem)

    def end_block(i, mid_ref):
        total = mid_ref[...].astype(F32) + bc2[...] + acc[...] + narrow(3, actb)
        xv[pl.ds(2 * i, 2)] = total.astype(BF16).reshape(2, 128, 512)

    def channel_mix(i, mine, ahead):
        (v_ref, mid_ref), (v_next, mid_next) = mine, ahead
        widen(1, v_ref, preb)
        bend(0, prea, acta)
        widen(2, v_ref, prea)
        token_half(jnp.minimum(i + 1, BLOCKS - 1), v_next, mid_next)
        acc[...] = narrow(0, acta)
        bend(1, preb, actb)
        widen(3, v_ref, preb)
        acc[...] += narrow(1, actb)
        bend(2, prea, acta)
        widen(0, v_next, prea)
        acc[...] += narrow(2, acta)
        bend(3, preb, actb)
        end_block(i, mid_ref)
        store(i).start()

    barrier = pltpu.get_barrier_semaphore()
    peers = group + [near[a][s] for a in "yz" for s in (1, 2, 3)]
    for peer in peers:
        pl.semaphore_signal(barrier, inc=1, device_id={"sp": peer}, device_id_type=MESH)
    start(early + loads[:1] + middle + loads[1:] + late)
    for load in early:
        load.wait()
    norm(0)
    w1o[...] = w1v[...].T
    pl.semaphore_wait(barrier, len(peers))
    pieces[0].pair.start()
    for a in rings:
        start(w1_ring[a])
    row = lax.broadcasted_iota(jnp.int32, (16, 128), 0)
    tile_in[8] = jnp.where(row == 2 * slot, b1_ref[0], jnp.where(row == 2 * slot + 1, b1_ref[1], 0.0))
    tile_in[slot] = tile_in[8]
    start(b1_group)
    start([w1_mine[a] for a in rings])
    for i, a in enumerate(rings):
        w1t[i, :, lanes(co[a], core)] = w1o[...]
    for load in middle:
        load.wait()
    w2t[...] = w2v[...].T
    b2c[...] = jnp.broadcast_to(b2[...], (128, 128)).T

    def later_norm(j):
        norm(j)
        pieces[j].pair.start()

    def w1_pass():
        for a in rings:
            for came, go in zip(w1_ring[a], w1_share[a]):
                came.wait_recv()
                go.start()
        arrive(b1_group)
        tile = tile_in[0]
        for n in range(1, 8):
            tile = tile + tile_in[n]
        tile_all[co["z"], co["y"]] = tile
        start(b1_y)

    def w1_end():
        for a in rings:
            arrive([w1_mine[a]] + w1_share[a])
        arrive(b1_y)
        start(b1_z)

    def b1_end():
        arrive(b1_z)

    def run(ops):
        for n, j in zip(ops[::2], ops[1::2]):
            j = int(j)
            if n in NAMES:
                STEPS[NAMES.index(n)](j, pieces[j])
            else:
                {"n": lambda: later_norm(j), "w": w1_pass, "v": w1_end, "u": b1_end}[n]()

    slots = {n: ops for n, ops in enumerate(ORDER) if ops}
    for ops in slots.pop(0):
        run(ops)
    for load in late:
        load.wait()
    token_half(0, va, mida)
    widen(0, va, prea)

    def loop(p, carry):
        for side, (mine, ahead) in enumerate((((va, mida), (vb, midb)), ((vb, midb), (va, mida)))):
            for n, ops in slots.items():
                if n % 2 == 1 - side:
                    @pl.when(p == (n - 1) // 2)
                    def _(ops=ops):
                        run(ops)
            channel_mix(2 * p + side, mine, ahead)
        return carry

    lax.fori_loop(0, BLOCKS // 2, loop, 0)
    local(xv, z_hbm, out_sem).wait()
    for copy in sent:
        copy.wait_send()


RINGS = len({axes[0] for axes, _ in PIECES})
N_COPIES = 31 * N + 7 * RINGS + 7 + 3 + 3


def vmem(*shape, dtype=BF16):
    return pltpu.VMEM(shape, dtype)


def mixer(x, w1, b1, w2, b2, wc1, bc1, wc2, bc2, g1, h1, g2, h2):
    any_space = pl.BlockSpec(memory_space=pl.ANY)
    scalars = pl.BlockSpec(memory_space=pltpu.SMEM)
    return pl.pallas_call(
        mixer_kernel,
        name="mixer",
        out_shape=jax.ShapeDtypeStruct((32, 128, 512), BF16),
        in_specs=[any_space, any_space, scalars] + [any_space] * 10,
        out_specs=any_space,
        scratch_shapes=[
            vmem(32, 128, 512),
            vmem(128, 256),
            vmem(256, 128),
            *[vmem(1, 512, dtype=F32)] * 5,
            vmem(1, 128, dtype=F32),
            vmem(1, 2048, dtype=F32),
            vmem(256, 128),
            vmem(RINGS, 256, 1024),
            vmem(128, 256),
            vmem(128, 128, dtype=F32),
            vmem(512, 2048),
            vmem(2048, 512),
            vmem(9, 16, 128, dtype=F32),
            vmem(4, 4, 16, 128, dtype=F32),
            vmem(N, 4, 128, 256),
            vmem(N, 4, 2, 128, 256),
            vmem(N, 4, 2, 128, 256),
            vmem(N, 2, 2, 128, 128),
            vmem(N, 4, 4, 16, 256, dtype=F32),
            vmem(N, 2, 4, 16, 128, dtype=F32),
            vmem(N, 2, 4, 16, 128, dtype=F32),
            vmem(N, 2, 4, 16, 128, dtype=F32),
            vmem(N, 4, 16, 256, dtype=F32),
            vmem(N, 4, 16, 256, dtype=F32),
            vmem(N, 2, 4, 4, 4, 16, 256),
            vmem(256, 512),
            vmem(256, 512),
            vmem(256, 512),
            vmem(256, 512),
            vmem(256, 512, dtype=F32),
            vmem(256, 512, dtype=F32),
            vmem(256, 512),
            vmem(256, 512),
            vmem(256, 512, dtype=F32),
            pltpu.SemaphoreType.DMA((N_COPIES,)),
            pltpu.SemaphoreType.DMA((N_COPIES,)),
            pltpu.SemaphoreType.DMA((N + 12,)),
        ],
        compiler_params=pltpu.CompilerParams(
            collective_id=0, has_side_effects=True, vmem_limit_bytes=60 * 1024 * 1024
        ),
    )(x, w1, b1, w2, *(v.reshape(1, -1) if v.ndim == 1 else v for v in (b2, wc1, bc1, wc2, bc2, g1, h1, g2, h2)))


def solution(mesh):
    row_spec = P("dp", "sp", None)
    in_specs = (row_spec, P("sp", None), P("sp"), P(None, "sp"), P("sp"), P(None, None), P(None), P(None, None), P(None), P(None), P(None), P(None), P(None))
    return jax.shard_map(mixer, mesh=mesh, in_specs=in_specs, out_specs=row_spec, check_vma=False)
```
